1024 devices in a mesh: gx: 64 (over z_lo, x, core), gy: 16 (over y, z_hi).
Axes of the slice: x: 4, y: 4, z: 32 (z_hi: 4, z_lo: 8; z = z_hi * 8 + z_lo), core: 2. Of those that a mesh axis runs over, the one named last changes fastest.
Arguments:
- prefix_tokens: bfloat16 [49152, 8192], P('gx'), may hold values from -6 to 6
- key_value_weight: bfloat16 [8192, 2048], P('gx', 'gy'), may hold values from -0.0625 to 0.0625
- prefix_lengths: int32 [384], P('gx'), may hold values from 1 to 128, as said below
- start_offsets: int32 [384], P('gx'), may hold values from 0 to 8064
- queries: bfloat16 [32, 8192], P('gy'), may hold values from -5 to 5
- key_value_cache: bfloat16 [2, 32, 8192, 1024], P(None, 'gy', 'gx'), may hold values from -5 to 5
- cache_lengths: int32 [32], P('gy'), may hold values from 1024 to 8192, as said below
- out_weight: bfloat16 [8192, 8192], P('gy', 'gx'), may hold values from -0.5 to 0.5
Outputs:
- prefix_kv: bfloat16 [49152, 2048], P('gx', 'gy')
- decode_out: bfloat16 [32, 8192], P('gy', 'gx')
The draws below stay inside these ranges and needn't reach their ends.
Inputs may be any that keep to these rules, and one draw needn't show every extreme that they name: `prefix_lengths`: live tokens stand at the front of a prefix's slots; in every draw some prefix uses all 128 slots. `cache_lengths`: live positions stand at the front of a trajectory's cache; in every draw some trajectory uses all 8192 positions.
All inputs are finite; a program needn't handle non-finite values.
Results may differ from the reference program's by a relative error of at most 0.0051.
Values may be sent and summed in bfloat16 or wider, within the bound.
No kernel may reach another device: no remote copies, remote signals or barrier semaphores. Data moves between devices by JAX's collectives and lax.ppermute only.
A program may use at most 64 MiB of HBM per device.

```python
import jax
import jax.numpy as jnp
from jax import lax

MODEL_WIDTH = 8192
QUERY_HEADS = 64
KEY_VALUE_HEADS = 8
HEAD_SIZE = 128
SLOT = 128
CACHE_PER_SHARD = 128
SEQS = 384
TOKENS = 49152
TRAJECTORY_COUNT = 32
CACHE_LENGTH = 8192
N_GX = 64


def draw_queries(key, part):
    base_key = jax.random.fold_in(key, 21)
    value_rows = jnp.clip(2.0 * jax.random.normal(base_key, (TRAJECTORY_COUNT, QUERY_HEADS * HEAD_SIZE), jnp.float32), -5.0, 5.0)
    return value_rows.astype(jnp.bfloat16)


def draw_key_value_cache(key, part):
    base_key = jax.random.fold_in(key, 22)
    array_shape = (2, TRAJECTORY_COUNT, CACHE_LENGTH, KEY_VALUE_HEADS * HEAD_SIZE)
    value_rows = jnp.clip(jax.random.normal(base_key, array_shape, jnp.float32), -5.0, 5.0)
    return value_rows.astype(jnp.bfloat16)


def draw_cache_lengths(key, part):
    lengths = jax.random.randint(jax.random.fold_in(key, 31), (TRAJECTORY_COUNT,), CACHE_LENGTH // 8, CACHE_LENGTH + 1)
    full_index = jax.random.randint(jax.random.fold_in(key, 32), (), 0, TRAJECTORY_COUNT)
    short_value = jax.random.randint(jax.random.fold_in(key, 33), (), CACHE_LENGTH // 8, CACHE_LENGTH)
    lengths = lengths.at[(full_index + 1) % TRAJECTORY_COUNT].set(short_value)
    return lengths.at[full_index].set(CACHE_LENGTH).astype(jnp.int32)


def draw_prefix_lengths(key, part):
    lengths = jax.random.randint(jax.random.fold_in(key, 41), (SEQS,), 1, SLOT + 1)
    full_index = jax.random.randint(jax.random.fold_in(key, 42), (), 0, SEQS)
    short_value = jax.random.randint(jax.random.fold_in(key, 43), (), 1, SLOT)
    lengths = lengths.at[(full_index + 1) % SEQS].set(short_value)
    return lengths.at[full_index].set(SLOT).astype(jnp.int32)


def plant(entries, stream_key, low, top_value):
    dims = entries.shape
    index_at = [jax.random.randint(jax.random.fold_in(stream_key, axis), (), 0, dims[axis]) for axis in range(len(dims))]
    entries = entries.at[tuple(index_at)].set(low)
    longest = dims.index(max(dims))
    index_at[longest] = (index_at[longest] + 1) % dims[longest]
    return entries.at[tuple(index_at)].set(top_value)


def shard_levels(rng, shape, pieces, least, top_value):
    loudness = 1.0
    for dim, shards_of in pieces:
        heights = jax.random.uniform(jax.random.fold_in(jax.random.fold_in(rng, 6), dim), (shards_of,), jnp.float32, least / len(pieces), top_value / len(pieces))
        loudness = loudness * jnp.repeat(jnp.exp(heights), shape[dim] // shards_of).reshape((-1,) + (1,) * (len(shape) - 1 - dim))
    return loudness


def bell_draw(own_key, extent, spread, limit, shards=(), held_as=jnp.bfloat16):
    array = jax.random.normal(own_key, extent, jnp.float32) * spread
    if len(shards) > 0:
        array = shard_levels(own_key, extent, shards, -0.22, 0.18) * array
    return jnp.clip(array, min=-limit, max=limit).astype(held_as)


def setup_inputs(seed: int = 0) -> dict:
    streams_of = jax.random.split(jax.random.key(seed), 9)
    prefix_tokens = bell_draw(streams_of[0], (TOKENS, MODEL_WIDTH), 1.0, 6.0, ((0, 64),))
    key_value_weight = bell_draw(streams_of[1], (MODEL_WIDTH, 2 * KEY_VALUE_HEADS * HEAD_SIZE), MODEL_WIDTH ** -0.5, 0.0625, ((0, 64), (1, 16)))
    prefix_lengths = draw_prefix_lengths(jax.random.fold_in(streams_of[8], 71), 0)
    start_offsets = plant(jax.random.randint(streams_of[3], (SEQS,), 0, CACHE_LENGTH - SLOT + 1), jax.random.fold_in(streams_of[3], 1), 0, CACHE_LENGTH - SLOT).astype(jnp.int32)
    queries = draw_queries(jax.random.fold_in(streams_of[8], 71), 0)
    key_value_cache = draw_key_value_cache(jax.random.fold_in(streams_of[8], 71), 0)
    cache_lengths = draw_cache_lengths(jax.random.fold_in(streams_of[8], 71), 0)
    out_weight = bell_draw(streams_of[7], (QUERY_HEADS * HEAD_SIZE, MODEL_WIDTH), (QUERY_HEADS * HEAD_SIZE // 64) ** -0.5, 0.5, ((0, 16), (1, 64)))
    return {"prefix_tokens": prefix_tokens, "key_value_weight": key_value_weight, "prefix_lengths": prefix_lengths, "start_offsets": start_offsets, "queries": queries, "key_value_cache": key_value_cache, "cache_lengths": cache_lengths, "out_weight": out_weight}


rope_base = 500000.0
masked_score = -1e30


def rotate_and_mask(projected, first_column, prefix_lengths, start_offsets):
    tok_rows, columns = projected.shape
    slot_index = jnp.arange(SLOT, dtype=jnp.int32)
    positions = (start_offsets[:, None] + slot_index[None, :]).reshape(tok_rows)
    live_rows = (slot_index[None, :] < prefix_lengths[:, None]).reshape(tok_rows)
    half_width = HEAD_SIZE // 2
    freq_index = jnp.arange(half_width, dtype=jnp.float32)
    inverse = rope_base ** (-2.0 * freq_index / HEAD_SIZE)
    angles = positions.astype(jnp.float32)[:, None] * inverse[None, :]
    cosine = jnp.cos(angles)[:, None, :]
    sine = jnp.sin(angles)[:, None, :]
    head_list = projected.reshape(tok_rows, columns // HEAD_SIZE, HEAD_SIZE)
    first_half = head_list[:, :, :half_width]
    second_half = head_list[:, :, half_width:]
    rotary_applied = jnp.concatenate([first_half * cosine - second_half * sine, second_half * cosine + first_half * sine], axis=2)
    head_position = first_column // HEAD_SIZE + jnp.arange(columns // HEAD_SIZE, dtype=jnp.int32)
    key_tagged = jnp.where((head_position < KEY_VALUE_HEADS)[None, :, None], rotary_applied, head_list)
    kept = jnp.where(live_rows[:, None, None], key_tagged, 0.0)
    return kept.reshape(tok_rows, columns).astype(jnp.bfloat16)


def attend_one(query_vector, cache_entry_row, length):
    query_group = QUERY_HEADS // KEY_VALUE_HEADS
    query_head_rows = query_vector.astype(jnp.float32).reshape(KEY_VALUE_HEADS, query_group, HEAD_SIZE)
    key_rows = cache_entry_row[0].astype(jnp.float32).reshape(N_GX, CACHE_PER_SHARD, KEY_VALUE_HEADS, HEAD_SIZE)
    value_rows = cache_entry_row[1].astype(jnp.float32).reshape(N_GX, CACHE_PER_SHARD, KEY_VALUE_HEADS, HEAD_SIZE)
    scores = jnp.einsum("hgd,kphd->khgp", query_head_rows, key_rows, precision=lax.Precision.HIGHEST) * (HEAD_SIZE ** -0.5)
    position = jnp.arange(CACHE_LENGTH, dtype=jnp.int32).reshape(N_GX, 1, 1, CACHE_PER_SHARD)
    valid = position < length
    peak = jnp.max(jnp.where(valid, scores, masked_score), axis=3)
    weights = jnp.where(valid, jnp.exp(scores - peak[..., None]), 0.0)
    block_total = jnp.sum(weights, axis=3)
    rounded = lax.optimization_barrier(weights.astype(jnp.bfloat16)).astype(jnp.float32)
    numerator = jnp.einsum("khgp,kphd->khgd", rounded, value_rows, precision=lax.Precision.HIGHEST)
    highest = jnp.max(peak, axis=0)
    factor = jnp.exp(peak - highest[None])
    denominator = jnp.sum(block_total * factor, axis=0)
    combined = jnp.sum(numerator * factor[..., None], axis=0)
    return (combined / denominator[..., None]).reshape(QUERY_HEADS * HEAD_SIZE).astype(jnp.bfloat16)


def reference(prefix_tokens, key_value_weight, prefix_lengths, start_offsets, queries, key_value_cache, cache_lengths, out_weight):
    projected = jnp.dot(prefix_tokens, key_value_weight, preferred_element_type=jnp.float32)
    prefix_kv = rotate_and_mask(projected, 0, prefix_lengths, start_offsets)

    def one_trajectory(index):
        cache_entry_row = lax.dynamic_index_in_dim(key_value_cache, index, 1, keepdims=False)
        return attend_one(queries[index], cache_entry_row, cache_lengths[index])

    attention = lax.map(one_trajectory, jnp.arange(TRAJECTORY_COUNT, dtype=jnp.int32))
    decode_out = jnp.dot(attention, out_weight, preferred_element_type=jnp.float32).astype(jnp.bfloat16)
    return prefix_kv, decode_out
```

```python
import jax
import jax.numpy as jnp
from jax import lax
from jax.experimental import pallas as pl
from jax.experimental.pallas import tpu as pltpu
from jax.sharding import Mesh
from jax.sharding import PartitionSpec as P

QUERY_HEADS = 64
KEY_VALUE_HEADS = 8
HEAD_SIZE = 128
SLOT = 128
GX = ("z", "x", "c")
GY = ("y", "w")
GROUP = QUERY_HEADS // KEY_VALUE_HEADS

rope_base = 500000.0
masked_score = -1e30


def swap(pieces, axis):
    return lax.all_to_all(pieces, axis, 0, 0, tiled=True)


def rotation(column, prefix_lengths, start_offsets):
    slot_index = jnp.arange(SLOT, dtype=jnp.int32)
    positions = (start_offsets[:, None] + slot_index[None, :]).reshape(-1, 1)
    live = (slot_index[None, :] < prefix_lengths[:, None]).reshape(-1, 1)
    half_width = HEAD_SIZE // 2
    lane = jnp.arange(HEAD_SIZE, dtype=jnp.int32)
    frequency = (lane % half_width).astype(jnp.float32)
    inverse = rope_base ** (-2.0 * frequency / HEAD_SIZE)
    angles = positions.astype(jnp.float32) * inverse[None, :]
    is_key = column < KEY_VALUE_HEADS
    sine = jnp.where(lane[None, :] < half_width, -jnp.sin(angles), jnp.sin(angles))
    along = jnp.where(live, jnp.where(is_key, jnp.cos(angles), 1.0), 0.0)
    across = jnp.where(live & is_key, sine, 0.0)
    return along, across


def packed(peak, total):
    lane = lax.broadcasted_iota(jnp.int32, (peak.shape[0], HEAD_SIZE), 1)
    return jnp.where(lane < HEAD_SIZE // 2, peak, total)


def block_kernel(limits_ref, query_ref, cache_ref, out_ref):
    trajectories, positions = cache_ref.shape[1], cache_ref.shape[2]
    position = lax.broadcasted_iota(jnp.int32, (GROUP, positions), 1)
    for t in range(trajectories):
        valid = position < limits_ref[t]
        for g in range(KEY_VALUE_HEADS):
            columns = slice(g * HEAD_SIZE, (g + 1) * HEAD_SIZE)
            scores = lax.dot_general(
                query_ref[t, g * GROUP : (g + 1) * GROUP, :],
                cache_ref[0, t, :, columns],
                (((1,), (1,)), ((), ())),
                preferred_element_type=jnp.float32,
            ) * HEAD_SIZE ** (-0.5)
            peak = jnp.max(jnp.where(valid, scores, masked_score), axis=1, keepdims=True)
            weights = jnp.where(valid, jnp.exp(scores - peak), 0.0)
            total = jnp.sum(weights, axis=1, keepdims=True)
            values = jnp.dot(
                weights.astype(jnp.bfloat16),
                cache_ref[1, t, :, columns],
                preferred_element_type=jnp.float32,
            )
            stats = packed(peak, total)
            for i in range(4):
                slot, row, pair = t * 4 + i, g * 2, slice(i * 2, i * 2 + 2)
                out_ref[slot, row : row + 2, :] = values[pair]
                out_ref[slot, 16 + row : 18 + row, :] = stats[pair]


def merged(parts):
    numerator, stats = parts[:, :16, :], parts[:, 16:, :]
    peak = stats[:, :, :1]
    total = stats[:, :, HEAD_SIZE // 2 : HEAD_SIZE // 2 + 1]
    top = jnp.max(peak, axis=0)
    factor = jnp.exp(peak - top[None])
    return top, jnp.sum(total * factor, axis=0), jnp.sum(numerator * factor, axis=0)


def merge_kernel(parts_ref, out_ref):
    top, total, numerator = merged(parts_ref[...])
    stats = packed(top, total)
    for k in range(out_ref.shape[0]):
        out_ref[k, :16, :] = numerator
        out_ref[k, 16:, :] = stats


def finish_kernel(parts_ref, out_ref):
    _, total, numerator = merged(parts_ref[...])
    attention = (numerator / total).astype(jnp.bfloat16).astype(jnp.float32)
    for k in range(out_ref.shape[0]):
        out_ref[k] = attention


def out_kernel(heads_ref, weight_ref, out_ref):
    trajectories = out_ref.shape[1]
    for t in range(trajectories):
        total = jnp.zeros((heads_ref.shape[1], HEAD_SIZE), jnp.float32)
        for i in range(4):
            total += jnp.dot(
                heads_ref[t * 4 + i].astype(jnp.bfloat16),
                weight_ref[i * HEAD_SIZE : (i + 1) * HEAD_SIZE, :],
                preferred_element_type=jnp.float32,
            )
        out_ref[:, t, :] = total


def prefill_kernel(place_ref, *refs):
    tokens, (own_ref, other_ref, along_ref, across_ref, out_ref, total_ref) = refs[:4], refs[4:]
    step = pl.program_id(0)

    @pl.when(step == 0)
    def _():
        total_ref[...] = jnp.zeros_like(total_ref)

    first = place_ref[2] == 0
    total = total_ref[...]
    for k, token_ref in enumerate(tokens):
        own, other = own_ref[k, 0], other_ref[k, 0]
        rows = jnp.concatenate(
            [jnp.where(first, own, other), jnp.where(first, other, own)], axis=0
        )
        total += jnp.dot(token_ref[...], rows, preferred_element_type=jnp.float32)
    total_ref[...] = total

    @pl.when(step == pl.num_programs(0) - 1)
    def _():
        swapped = pltpu.roll(total, HEAD_SIZE // 2, 1)
        rotated = total * along_ref[...] + swapped * across_ref[...]
        out_ref[...] = rotated.astype(jnp.bfloat16)


def prefill(place, tokens, own, other, along, across):
    rows, columns = tokens.shape[0], own.shape[-1]
    nx, nz = own.shape[:2]

    def token_block(k):
        def index(step, place):
            flipped = (step & 1) * 4 + (step & 2) + (step >> 2)
            return 0, (place[0] ^ flipped) * nx + ((place[1] + nx - k) & (nx - 1))

        return index

    whole = pl.BlockSpec((rows, columns), lambda step, place: (0, 0))
    piece = pl.BlockSpec((nx, 1, *own.shape[2:]), lambda step, place: (0, step, 0, 0))
    return pl.pallas_call(
        prefill_kernel,
        out_shape=jax.ShapeDtypeStruct((rows, columns), jnp.bfloat16),
        grid_spec=pltpu.PrefetchScalarGridSpec(
            num_scalar_prefetch=1,
            grid=(nz,),
            in_specs=[pl.BlockSpec((rows, 2 * HEAD_SIZE), token_block(k)) for k in range(nx)]
            + [piece, piece, whole, whole],
            out_specs=whole,
            scratch_shapes=[pltpu.VMEM((rows, columns), jnp.float32)],
        ),
        cost_estimate=pl.CostEstimate(
            flops=2 * 10**9, bytes_accessed=2 * tokens.size, transcendentals=0
        ),
    )(place, *([tokens] * nx), own, other, along, across)


VMEM = pl.BlockSpec(memory_space=pltpu.VMEM)
SMEM = pl.BlockSpec(memory_space=pltpu.SMEM)


def whole_call(kernel, shape, in_specs=(VMEM,), flops=10**7):
    return pl.pallas_call(
        kernel,
        out_shape=jax.ShapeDtypeStruct(shape, jnp.float32),
        in_specs=list(in_specs),
        out_specs=VMEM,
        cost_estimate=pl.CostEstimate(flops=flops, bytes_accessed=2**20, transcendentals=0),
    )


def shards(
    prefix_tokens,
    key_value_weight,
    prefix_lengths,
    start_offsets,
    queries,
    key_value_cache,
    cache_lengths,
    out_weight,
):
    columns = key_value_weight.shape[1]
    nz, nx, nc, ny, nw = (lax.axis_size(a) for a in ("z", "x", "c", "y", "w"))
    nxc, ngy = nx * nc, ny * nw

    blocks = key_value_weight[None]
    for far in (4, 2, 1):
        other = lax.ppermute(blocks, "z", [(i, i ^ far) for i in range(nz)])
        blocks = jnp.concatenate([blocks, other], axis=0)
    sides = [blocks]
    for k in range(1, nx):
        sides.append(lax.ppermute(blocks, "x", [(i, (i + k) % nx) for i in range(nx)]))
    own = jnp.stack(sides)
    other = lax.ppermute(own, "c", [(0, 1), (1, 0)])
    place = jnp.stack([lax.axis_index(a) for a in GX]).astype(jnp.int32)
    along, across = rotation(lax.axis_index(GY), prefix_lengths, start_offsets)
    prefix_kv = prefill(place, prefix_tokens, own, other, along, across)

    trajectories = queries.shape[0]
    cache_per_shard = key_value_cache.shape[2]
    limits = cache_lengths - lax.axis_index(GX) * cache_per_shard
    ordered = queries.reshape(trajectories, KEY_VALUE_HEADS, 2, 4, HEAD_SIZE)
    ordered = ordered.swapaxes(2, 3).reshape(trajectories, QUERY_HEADS, HEAD_SIZE)
    parts = whole_call(
        block_kernel, (nxc, 32, HEAD_SIZE), (SMEM, VMEM, VMEM), flops=10**9
    )(limits, ordered, key_value_cache)
    parts = swap(parts, ("x", "c"))
    parts = whole_call(merge_kernel, (nz, 32, HEAD_SIZE))(parts)
    parts = swap(parts, "z")
    attention = whole_call(finish_kernel, (nxc, ngy, HEAD_SIZE))(parts)
    heads = swap(attention.reshape(nxc * ngy, 1, HEAD_SIZE), ("x", "c", *GY))
    mixed = whole_call(out_kernel, (ngy, trajectories, columns), (VMEM, VMEM))(
        heads.reshape(nxc, ngy, HEAD_SIZE), out_weight
    )
    mixed = swap(mixed, GY)
    return (prefix_kv, jnp.sum(mixed, axis=0).astype(jnp.bfloat16))


def solution(mesh):
    finer = Mesh(mesh.devices.reshape(8, 4, 2, 4, 4), ("z", "x", "c", "y", "w"))
    return jax.shard_map(
        shards,
        mesh=finer,
        in_specs=(
            P(GX, None),
            P(GX, GY),
            P(GX),
            P(GX),
            P(GY, None),
            P(None, GY, GX, None),
            P(GY),
            P(GY, GX),
        ),
        out_specs=(P(GX, GY), P(GY, GX)),
        check_vma=False,
    )
```

```python
import jax
import jax.numpy as jnp
import numpy as np
from jax import lax
from jax.experimental import pallas as pl
from jax.experimental.pallas import tpu as pltpu
from jax.sharding import Mesh
from jax.sharding import PartitionSpec as P

QUERY_HEADS = 64
KEY_VALUE_HEADS = 8
HEAD_SIZE = 128
SLOT = 128
GX = ("z", "x", "c")
GY = ("y", "w")
GROUP = QUERY_HEADS // KEY_VALUE_HEADS

rope_base = 500000.0
masked_score = -1e30


def swap(pieces, axis):
    return lax.all_to_all(pieces, axis, 0, 0, tiled=True)


def turns():
    half_width = HEAD_SIZE // 2
    inverse = rope_base ** (-2.0 * (np.arange(HEAD_SIZE) % half_width) / HEAD_SIZE)
    angles = np.arange(SLOT)[:, None] * inverse[None, :]
    return tuple(np.float32(table) for table in (inverse, np.cos(angles), np.sin(angles)))


def packed(peak, total):
    lane = lax.broadcasted_iota(jnp.int32, (peak.shape[0], HEAD_SIZE), 1)
    return jnp.where(lane < HEAD_SIZE // 2, peak, total)


def block_kernel(place_ref, limits_ref, query_ref, cache_ref, out_ref):
    trajectories, positions = cache_ref.shape[1], cache_ref.shape[2]
    side = place_ref[2]
    pairs = [(t, g) for t in range(trajectories) for g in range(KEY_VALUE_HEADS)]
    columns = [slice(g * HEAD_SIZE, (g + 1) * HEAD_SIZE) for g in range(KEY_VALUE_HEADS)]
    scores = jnp.concatenate(
        [
            lax.dot_general(
                query_ref[t, g * GROUP : (g + 1) * GROUP, :],
                cache_ref[0, t, :, columns[g]],
                (((1,), (1,)), ((), ())),
                preferred_element_type=jnp.float32,
            )
            for t, g in pairs
        ],
        axis=0,
    ) * HEAD_SIZE ** (-0.5)
    position = lax.broadcasted_iota(jnp.int32, (QUERY_HEADS, positions), 1)
    valid = jnp.concatenate([position < limits_ref[t] for t in range(trajectories)], axis=0)
    peak = jnp.max(jnp.where(valid, scores, masked_score), axis=1, keepdims=True)
    weights = jnp.where(valid, jnp.exp(scores - peak), 0.0)
    stats = packed(peak, jnp.sum(weights, axis=1, keepdims=True))
    for k, (t, g) in enumerate(pairs):
        rows = slice(k * GROUP, (k + 1) * GROUP)
        values = jnp.dot(
            weights[rows].astype(jnp.bfloat16),
            cache_ref[1, t, :, columns[g]],
            preferred_element_type=jnp.float32,
        )
        for half in range(2):
            kept, slot, row = half ^ side, t * 2 + g % 2, (g // 2) * 4
            some = slice(half * 4, half * 4 + 4)
            out_ref[kept, slot, row : row + 4, :] = values[some]
            out_ref[kept, slot, 16 + row : 20 + row, :] = stats[rows][some]


def merged(one, two):
    half_width = HEAD_SIZE // 2
    peaks = [part[16:, :1] for part in (one, two)]
    totals = [part[16:, half_width : half_width + 1] for part in (one, two)]
    top = jnp.maximum(*peaks)
    factors = [jnp.exp(peak - top) for peak in peaks]
    total = totals[0] * factors[0] + totals[1] * factors[1]
    return top, total, one[:16] * factors[0] + two[:16] * factors[1]


def store_merged(out_ref, index, one, two):
    top, total, numerator = merged(one, two)
    out_ref[(*index, slice(0, 16))] = numerator
    out_ref[(*index, slice(16, 32))] = packed(top, total)


def merge_pairs_kernel(place_ref, mine_ref, other_ref, out_ref):
    for slot in range(4):
        index = (slot & 1) ^ (place_ref[1] & 1), slot >> 1
        store_merged(out_ref, index, mine_ref[0, slot], other_ref[slot])


def merge_sides_kernel(place_ref, mine_ref, other_ref, out_ref):
    for slot in range(2):
        index = (slot ^ (place_ref[1] >> 1),)
        store_merged(out_ref, index, mine_ref[0, slot], other_ref[slot])


def merge_last_kernel(mine_ref, other_ref, out_ref):
    store_merged(out_ref, (), mine_ref[0], other_ref[...])


def merge_kernel(mine_ref, other_ref, out_ref):
    store_merged(out_ref, (), mine_ref[...], other_ref[...])


def finish_kernel(mine_ref, other_ref, out_ref):
    _, total, numerator = merged(mine_ref[...], other_ref[...])
    attention = (numerator / total).astype(jnp.bfloat16).astype(jnp.float32)
    for k in range(out_ref.shape[0]):
        out_ref[k] = attention


def out_kernel(heads_ref, weight_ref, out_ref):
    ny, trajectories = out_ref.shape[:2]
    total = jnp.zeros((trajectories * ny, HEAD_SIZE), jnp.float32)
    for quarter in range(4):
        heads = [
            jnp.concatenate(
                [
                    heads_ref[pl.ds((t * 4 + quarter) * 4 * ny + i, ny, stride=4), :]
                    for t in range(trajectories)
                ],
                axis=0,
            )
            for i in range(4)
        ]
        total += jnp.dot(
            jnp.concatenate(heads, axis=1).astype(jnp.bfloat16),
            weight_ref[quarter],
            preferred_element_type=jnp.float32,
        )
    for t in range(trajectories):
        out_ref[:, t, :] = total[t * ny : (t + 1) * ny]


def prefill_kernel(place_ref, *refs):
    tokens, refs = refs[:4], refs[4:]
    own_ref, other_ref, live_ref, starts_ref, cosine_ref, sine_ref, out_ref, total_ref = refs
    step = pl.program_id(0)

    @pl.when(step == 0)
    def _():
        total_ref[...] = jnp.zeros_like(total_ref)

    first = place_ref[2] == 0
    total = total_ref[...]
    for k, token_ref in enumerate(tokens):
        own, other = own_ref[k, 0], other_ref[k, 0]
        rows = jnp.concatenate(
            [jnp.where(first, own, other), jnp.where(first, other, own)], axis=0
        )
        total += jnp.dot(token_ref[...], rows, preferred_element_type=jnp.float32)
    total_ref[...] = total

    @pl.when(step == pl.num_programs(0) - 1)
    def _():
        prefixes = starts_ref.shape[0] // 2
        slot = lax.broadcasted_iota(jnp.int32, (SLOT, HEAD_SIZE), 0)
        front = lax.broadcasted_iota(jnp.int32, (SLOT, HEAD_SIZE), 1) < HEAD_SIZE // 2
        for i in range(prefixes):
            rows = slice(i * SLOT, (i + 1) * SLOT)
            plain = total_ref[rows, :]
            along, across = starts_ref[i : i + 1, :], starts_ref[prefixes + i : prefixes + i + 1, :]
            cosine = cosine_ref[...] * along - sine_ref[...] * across
            sine = sine_ref[...] * along + cosine_ref[...] * across
            swapped = pltpu.roll(plain, HEAD_SIZE // 2, 1)
            turned = plain * cosine + swapped * jnp.where(front, -sine, sine)
            kept = jnp.where(place_ref[3] > 0, turned, plain)
            out_ref[rows, :] = jnp.where(slot < live_ref[i], kept, 0.0).astype(jnp.bfloat16)


def prefill(place, tokens, own, other, live, starts, cosine, sine):
    rows, columns = tokens.shape[0], own.shape[-1]
    nx, nz = own.shape[:2]

    def token_block(k):
        def index(step, place):
            flipped = (step & 1) * 4 + (step & 2) + (step >> 2)
            return 0, (place[0] ^ flipped) * nx + ((place[1] + nx - k) & (nx - 1))

        return index

    def whole(array):
        return pl.BlockSpec(array.shape, lambda step, place: (0, 0))

    piece = pl.BlockSpec((nx, 1, *own.shape[2:]), lambda step, place: (0, step, 0, 0))
    result = jax.ShapeDtypeStruct((rows, columns), jnp.bfloat16)
    return pl.pallas_call(
        prefill_kernel,
        out_shape=result,
        grid_spec=pltpu.PrefetchScalarGridSpec(
            num_scalar_prefetch=1,
            grid=(nz,),
            in_specs=[pl.BlockSpec((rows, 2 * HEAD_SIZE), token_block(k)) for k in range(nx)]
            + [piece, piece, SMEM, whole(starts), whole(cosine), whole(sine)],
            out_specs=whole(result),
            scratch_shapes=[pltpu.VMEM((rows, columns), jnp.float32)],
        ),
        cost_estimate=pl.CostEstimate(
            flops=2 * 10**9, bytes_accessed=2 * tokens.size, transcendentals=0
        ),
    )(place, *([tokens] * nx), own, other, live, starts, cosine, sine)


VMEM = pl.BlockSpec(memory_space=pltpu.VMEM)
SMEM = pl.BlockSpec(memory_space=pltpu.SMEM)


def whole_call(kernel, shape, in_specs=(VMEM,), flops=10**7):
    return pl.pallas_call(
        kernel,
        out_shape=jax.ShapeDtypeStruct(shape, jnp.float32),
        in_specs=list(in_specs),
        out_specs=VMEM,
        cost_estimate=pl.CostEstimate(flops=flops, bytes_accessed=2**20, transcendentals=0),
    )


def shards(
    prefix_tokens,
    key_value_weight,
    prefix_lengths,
    start_offsets,
    queries,
    key_value_cache,
    cache_lengths,
    out_weight,
):
    columns = key_value_weight.shape[1]
    nz, nx, nc, ny, nw = (lax.axis_size(a) for a in ("z", "x", "c", "y", "w"))
    nxc = nx * nc

    blocks = key_value_weight[None]
    for far in (4, 2, 1):
        other = lax.ppermute(blocks, "z", [(i, i ^ far) for i in range(nz)])
        blocks = jnp.concatenate([blocks, other], axis=0)
    sides = [blocks]
    for k in range(1, nx):
        sides.append(lax.ppermute(blocks, "x", [(i, (i + k) % nx) for i in range(nx)]))
    own = jnp.stack(sides)
    other = lax.ppermute(own, "c", [(0, 1), (1, 0)])
    column = lax.axis_index(GY)
    place = jnp.stack([*(lax.axis_index(a) for a in GX), KEY_VALUE_HEADS - column])
    inverse, cosine, sine = turns()
    angles = start_offsets.astype(jnp.float32)[:, None] * inverse[None, :]
    starts = jnp.concatenate([jnp.cos(angles), jnp.sin(angles)], axis=0)
    prefix_kv = prefill(
        place, prefix_tokens, own, other, prefix_lengths, starts, cosine, sine
    )

    out_rows = swap(jnp.broadcast_to(out_weight[None], (nw, *out_weight.shape)), "w")

    trajectories = queries.shape[0]
    cache_per_shard = key_value_cache.shape[2]
    limits = cache_lengths - lax.axis_index(GX) * cache_per_shard
    by_head = queries.reshape(trajectories, QUERY_HEADS, HEAD_SIZE)
    parts = whole_call(
        block_kernel, (2, nx, 32, HEAD_SIZE), (SMEM, SMEM, VMEM, VMEM), flops=10**9
    )(place, limits, by_head, key_value_cache)
    other = lax.ppermute(parts[1], "c", [(0, 1), (1, 0)])
    parts = whole_call(merge_pairs_kernel, (2, 2, 32, HEAD_SIZE), (SMEM, VMEM, VMEM))(
        place, parts, other
    )
    other = lax.ppermute(parts[1], "x", [(i, i ^ 1) for i in range(nx)])
    parts = whole_call(merge_sides_kernel, (2, 32, HEAD_SIZE), (SMEM, VMEM, VMEM))(
        place, parts, other
    )
    other = lax.ppermute(parts[1], "x", [(i, i ^ 2) for i in range(nx)])
    parts = whole_call(merge_last_kernel, (32, HEAD_SIZE), (VMEM, VMEM))(parts, other)
    other = lax.ppermute(parts, "z", [(i, i ^ 1) for i in range(nz)])
    parts = whole_call(merge_kernel, (32, HEAD_SIZE), (VMEM, VMEM))(parts, other)
    other = lax.ppermute(parts, "z", [(i, i ^ 2) for i in range(nz)])
    parts = whole_call(merge_kernel, (32, HEAD_SIZE), (VMEM, VMEM))(parts, other)
    other = lax.ppermute(parts, "z", [(i, i ^ 4) for i in range(nz)])
    attention = whole_call(finish_kernel, (nxc, 16, HEAD_SIZE), (VMEM, VMEM))(parts, other)
    heads = swap(attention.reshape(nxc * ny, 4, HEAD_SIZE), ("x", "c", "y"))
    mixed = whole_call(out_kernel, (ny, trajectories, columns), (VMEM, VMEM))(
        heads.reshape(nxc * ny * 4, HEAD_SIZE), out_rows
    )
    mixed = swap(mixed, "y")
    return (prefix_kv, jnp.sum(mixed, axis=0).astype(jnp.bfloat16))


def solution(mesh):
    finer = Mesh(mesh.devices.reshape(8, 4, 2, 4, 4), ("z", "x", "c", "y", "w"))
    return jax.shard_map(
        shards,
        mesh=finer,
        in_specs=(
            P(GX, None),
            P(GX, GY),
            P(GX),
            P(GX),
            P(GY, None),
            P(None, GY, GX, None),
            P(GY),
            P(GY, GX),
        ),
        out_specs=(P(GX, GY), P(GY, GX)),
        check_vma=False,
    )
```

```python
import jax
import jax.numpy as jnp
import numpy as np
from jax import lax
from jax.experimental import pallas as pl
from jax.experimental.pallas import tpu as pltpu
from jax.sharding import Mesh
from jax.sharding import PartitionSpec as P

QUERY_HEADS = 64
KEY_VALUE_HEADS = 8
HEAD_SIZE = 128
SLOT = 128
GX = ("z", "x", "c")
GY = ("y", "w")
GROUP = QUERY_HEADS // KEY_VALUE_HEADS

rope_base = 500000.0
masked_score = -1e30


def swap(pieces, axis):
    return lax.all_to_all(pieces, axis, 0, 0, tiled=True)


def turns():
    half_width = HEAD_SIZE // 2
    inverse = rope_base ** (-2.0 * (np.arange(HEAD_SIZE) % half_width) / HEAD_SIZE)
    angles = np.arange(SLOT)[:, None] * inverse[None, :]
    return tuple(np.float32(table) for table in (inverse, np.cos(angles), np.sin(angles)))


def block_kernel(place_ref, lengths_ref, query_ref, cache_ref, out_ref):
    trajectories, positions = cache_ref.shape[1], cache_ref.shape[2]
    start = place_ref[4] * positions
    pairs = [(t, g) for t in range(trajectories) for g in range(KEY_VALUE_HEADS)]
    columns = [slice(g * HEAD_SIZE, (g + 1) * HEAD_SIZE) for g in range(KEY_VALUE_HEADS)]
    scores = jnp.concatenate(
        [
            lax.dot_general(
                query_ref[t, g * GROUP : (g + 1) * GROUP, :],
                cache_ref[0, t, :, columns[g]],
                (((1,), (1,)), ((), ())),
                preferred_element_type=jnp.float32,
            )
            for t, g in pairs
        ],
        axis=0,
    ) * HEAD_SIZE ** (-0.5)
    position = start + lax.broadcasted_iota(jnp.int32, (QUERY_HEADS, positions), 1)
    valid = jnp.concatenate([position < lengths_ref[t] for t in range(trajectories)], axis=0)
    peak = jnp.max(jnp.where(valid, scores, masked_score), axis=1, keepdims=True)
    weights = jnp.where(valid, jnp.exp(scores - peak), 0.0)
    total = jnp.sum(weights, axis=1, keepdims=True)
    lane = lax.broadcasted_iota(jnp.int32, weights.shape, 1)
    stats = jnp.where(lane < HEAD_SIZE // 2, peak, total)
    for k, (t, g) in enumerate(pairs):
        rows = slice(k * GROUP, (k + 1) * GROUP)
        values = jnp.dot(
            weights[rows].astype(jnp.bfloat16),
            cache_ref[1, t, :, columns[g]],
            preferred_element_type=jnp.float32,
        )
        for i in range(4):
            owner, row, pair = (t * 4 + i) * 4 + g // 2, (g % 2) * 2, slice(i * 2, i * 2 + 2)
            out_ref[owner, row : row + 2, :] = values[pair]
            out_ref[owner, row + 4 : row + 6, :] = stats[rows][pair]


def merge_kernel(parts_ref, out_ref):
    ny = parts_ref.shape[1]
    lane = lax.broadcasted_iota(jnp.int32, (4, HEAD_SIZE), 1)
    merged = []
    for y in range(ny):
        numerator, stats = parts_ref[:, y, :4, :], parts_ref[:, y, 4:, :]
        peak, total = stats[:, :, :1], stats[:, :, HEAD_SIZE // 2 : HEAD_SIZE // 2 + 1]
        top = jnp.max(peak, axis=0)
        factor = jnp.exp(peak - top[None])
        total = jnp.sum(total * factor, axis=0)
        some = total > 0.0
        safe = jnp.where(some, total, 1.0)
        attention = jnp.sum(numerator * factor, axis=0) / safe
        weight = jnp.where(some, top + jnp.log(safe), masked_score)
        high = weight.astype(jnp.bfloat16).astype(jnp.float32)
        middle = (weight - high).astype(jnp.bfloat16).astype(jnp.float32)
        low = weight - high - middle
        weight = jnp.where(lane < 32, high, jnp.where(lane < 64, middle, low))
        merged.append((attention, weight))
    for w in range(4):
        rows = [part[w : w + 1] for kind in range(2) for part in (pair[kind] for pair in merged)]
        piece = jnp.concatenate(rows, axis=0).astype(jnp.bfloat16)
        for z in range(out_ref.shape[0]):
            out_ref[z, w] = piece


def finish_kernel(parts_ref, out_ref):
    for w in range(parts_ref.shape[1]):
        parts = parts_ref[:, w].astype(jnp.float32)
        attention, stats = parts[:, :4, :], parts[:, 4:, :]
        weight = stats[:, :, :1] + stats[:, :, 32:33] + stats[:, :, 64:65]
        factor = jnp.exp(weight - jnp.max(weight, axis=0)[None])
        rows = jnp.sum(attention * factor, axis=0) / jnp.sum(factor, axis=0)
        rows = rows.astype(jnp.bfloat16).astype(jnp.float32)
        for k in range(out_ref.shape[0]):
            out_ref[k, pl.ds(w, 4, stride=4), :] = rows


def out_kernel(heads_ref, weight_ref, out_ref):
    trajectories = out_ref.shape[1]
    for t in range(trajectories):
        total = jnp.zeros((heads_ref.shape[1], HEAD_SIZE), jnp.float32)
        for i in range(4):
            total += jnp.dot(
                heads_ref[t * 4 + i].astype(jnp.bfloat16),
                weight_ref[i * HEAD_SIZE : (i + 1) * HEAD_SIZE, :],
                preferred_element_type=jnp.float32,
            )
        out_ref[:, t, :] = total


def prefill_kernel(place_ref, *refs):
    tokens, refs = refs[:4], refs[4:]
    own_ref, other_ref, live_ref, starts_ref, cosine_ref, sine_ref, out_ref, total_ref = refs
    step = pl.program_id(0)

    @pl.when(step == 0)
    def _():
        total_ref[...] = jnp.zeros_like(total_ref)

    first = place_ref[2] == 0
    total = total_ref[...]
    for k, token_ref in enumerate(tokens):
        own, other = own_ref[k, 0], other_ref[k, 0]
        rows = jnp.concatenate(
            [jnp.where(first, own, other), jnp.where(first, other, own)], axis=0
        )
        total += jnp.dot(token_ref[...], rows, preferred_element_type=jnp.float32)
    total_ref[...] = total

    @pl.when(step == pl.num_programs(0) - 1)
    def _():
        prefixes = starts_ref.shape[0] // 2
        slot = lax.broadcasted_iota(jnp.int32, (SLOT, HEAD_SIZE), 0)
        front = lax.broadcasted_iota(jnp.int32, (SLOT, HEAD_SIZE), 1) < HEAD_SIZE // 2
        for i in range(prefixes):
            rows = slice(i * SLOT, (i + 1) * SLOT)
            plain = total_ref[rows, :]
            along, across = starts_ref[i : i + 1, :], starts_ref[prefixes + i : prefixes + i + 1, :]
            cosine = cosine_ref[...] * along - sine_ref[...] * across
            sine = sine_ref[...] * along + cosine_ref[...] * across
            swapped = pltpu.roll(plain, HEAD_SIZE // 2, 1)
            turned = plain * cosine + swapped * jnp.where(front, -sine, sine)
            kept = jnp.where(place_ref[3] > 0, turned, plain)
            out_ref[rows, :] = jnp.where(slot < live_ref[i], kept, 0.0).astype(jnp.bfloat16)


def prefill(place, tokens, own, other, live, starts, cosine, sine):
    rows, columns = tokens.shape[0], own.shape[-1]
    nx, nz = own.shape[:2]

    def token_block(k):
        def index(step, place):
            flipped = (step & 1) * 4 + (step & 2) + (step >> 2)
            return 0, (place[0] ^ flipped) * nx + ((place[1] + nx - k) & (nx - 1))

        return index

    def whole(array):
        return pl.BlockSpec(array.shape, lambda step, place: (0, 0))

    piece = pl.BlockSpec((nx, 1, *own.shape[2:]), lambda step, place: (0, step, 0, 0))
    result = jax.ShapeDtypeStruct((rows, columns), jnp.bfloat16)
    return pl.pallas_call(
        prefill_kernel,
        out_shape=result,
        grid_spec=pltpu.PrefetchScalarGridSpec(
            num_scalar_prefetch=1,
            grid=(nz,),
            in_specs=[pl.BlockSpec((rows, 2 * HEAD_SIZE), token_block(k)) for k in range(nx)]
            + [piece, piece, SMEM, whole(starts), whole(cosine), whole(sine)],
            out_specs=whole(result),
            scratch_shapes=[pltpu.VMEM((rows, columns), jnp.float32)],
        ),
        cost_estimate=pl.CostEstimate(
            flops=2 * 10**9, bytes_accessed=2 * tokens.size, transcendentals=0
        ),
    )(place, *([tokens] * nx), own, other, live, starts, cosine, sine)


VMEM = pl.BlockSpec(memory_space=pltpu.VMEM)
SMEM = pl.BlockSpec(memory_space=pltpu.SMEM)


def whole_call(kernel, shape, in_specs=(VMEM,), flops=10**7, dtype=jnp.float32):
    return pl.pallas_call(
        kernel,
        out_shape=jax.ShapeDtypeStruct(shape, dtype),
        in_specs=list(in_specs),
        out_specs=VMEM,
        cost_estimate=pl.CostEstimate(flops=flops, bytes_accessed=2**20, transcendentals=0),
    )


def shards(
    prefix_tokens,
    key_value_weight,
    prefix_lengths,
    start_offsets,
    queries,
    key_value_cache,
    cache_lengths,
    out_weight,
):
    columns = key_value_weight.shape[1]
    nz, nx, nc, ny, nw = (lax.axis_size(a) for a in ("z", "x", "c", "y", "w"))
    nxc, ngy = nx * nc, ny * nw

    blocks = key_value_weight[None]
    for far in (4, 2, 1):
        other = lax.ppermute(blocks, "z", [(i, i ^ far) for i in range(nz)])
        blocks = jnp.concatenate([blocks, other], axis=0)
    sides = [blocks]
    for k in range(1, nx):
        sides.append(lax.ppermute(blocks, "x", [(i, (i + k) % nx) for i in range(nx)]))
    own = jnp.stack(sides)
    other = lax.ppermute(own, "c", [(0, 1), (1, 0)])
    column = lax.axis_index(GY)
    place = jnp.stack(
        [*(lax.axis_index(a) for a in GX), KEY_VALUE_HEADS - column, lax.axis_index(GX)]
    )
    inverse, cosine, sine = turns()
    angles = start_offsets.astype(jnp.float32)[:, None] * inverse[None, :]
    starts = jnp.concatenate([jnp.cos(angles), jnp.sin(angles)], axis=0)
    prefix_kv = prefill(
        place, prefix_tokens, own, other, prefix_lengths, starts, cosine, sine
    )

    trajectories = queries.shape[0]
    ordered = queries.reshape(trajectories, KEY_VALUE_HEADS, 2, 4, HEAD_SIZE)
    ordered = ordered.swapaxes(2, 3).reshape(trajectories, QUERY_HEADS, HEAD_SIZE)
    parts = whole_call(
        block_kernel, (nxc * ny, 8, HEAD_SIZE), (SMEM, SMEM, VMEM, VMEM), flops=10**9
    )(place, cache_lengths, ordered, key_value_cache)
    parts = swap(parts, ("x", "c", "y"))
    parts = whole_call(merge_kernel, (nz, nw, 8, HEAD_SIZE), dtype=jnp.bfloat16)(
        parts.reshape(nxc, ny, 8, HEAD_SIZE)
    )
    parts = swap(parts.reshape(nz * nw, 8, HEAD_SIZE), ("z", "w"))
    attention = whole_call(finish_kernel, (nxc, ngy, HEAD_SIZE))(
        parts.reshape(nz, nw, 8, HEAD_SIZE)
    )
    heads = swap(attention, ("x", "c"))
    mixed = whole_call(out_kernel, (ngy, trajectories, columns), (VMEM, VMEM))(heads, out_weight)
    mixed = swap(mixed, GY)
    return (prefix_kv, jnp.sum(mixed, axis=0).astype(jnp.bfloat16))


def solution(mesh):
    finer = Mesh(mesh.devices.reshape(8, 4, 2, 4, 4), ("z", "x", "c", "y", "w"))
    return jax.shard_map(
        shards,
        mesh=finer,
        in_specs=(
            P(GX, None),
            P(GX, GY),
            P(GX),
            P(GX),
            P(GY, None),
            P(None, GY, GX, None),
            P(GY),
            P(GY, GX),
        ),
        out_specs=(P(GX, GY), P(GY, GX)),
        check_vma=False,
    )
```

```python
import jax
import jax.numpy as jnp
import numpy as np
from jax import lax
from jax.experimental import pallas as pl
from jax.experimental.pallas import tpu as pltpu
from jax.sharding import Mesh
from jax.sharding import PartitionSpec as P

QUERY_HEADS = 64
KEY_VALUE_HEADS = 8
HEAD_SIZE = 128
SLOT = 128
GX = ("z", "x", "c")
GY = ("y", "w")
GROUP = QUERY_HEADS // KEY_VALUE_HEADS

rope_base = 500000.0
masked_score = -1e30


def swap(pieces, axis):
    return lax.all_to_all(pieces, axis, 0, 0, tiled=True)


def turns():
    half_width = HEAD_SIZE // 2
    inverse = rope_base ** (-2.0 * (np.arange(HEAD_SIZE) % half_width) / HEAD_SIZE)
    angles = np.arange(SLOT)[:, None] * inverse[None, :]
    return tuple(np.float32(table) for table in (inverse, np.cos(angles), np.sin(angles)))


def block_kernel(place_ref, lengths_ref, query_ref, cache_ref, out_ref):
    trajectories, positions = cache_ref.shape[1], cache_ref.shape[2]
    start = place_ref[4] * positions
    pairs = [(t, g) for t in range(trajectories) for g in range(KEY_VALUE_HEADS)]
    columns = [slice(h * HEAD_SIZE, (h + 1) * HEAD_SIZE) for h in range(QUERY_HEADS)]
    queries = query_ref[...].astype(jnp.float32)
    order = [i + 4 * side for i in range(4) for side in range(2)]
    scores = jnp.concatenate(
        [
            lax.dot_general(
                jnp.concatenate(
                    [queries[t : t + 1, columns[g * GROUP + r]] for r in order], axis=0
                ).astype(jnp.bfloat16),
                cache_ref[0, t, :, columns[g]],
                (((1,), (1,)), ((), ())),
                preferred_element_type=jnp.float32,
            )
            for t, g in pairs
        ],
        axis=0,
    ) * HEAD_SIZE ** (-0.5)
    position = start + lax.broadcasted_iota(jnp.int32, (QUERY_HEADS, positions), 1)
    valid = jnp.concatenate([position < lengths_ref[t] for t in range(trajectories)], axis=0)
    peak = jnp.max(jnp.where(valid, scores, masked_score), axis=1, keepdims=True)
    weights = jnp.where(valid, jnp.exp(scores - peak), 0.0)
    total = jnp.sum(weights, axis=1, keepdims=True)
    lane = lax.broadcasted_iota(jnp.int32, weights.shape, 1)
    stats = jnp.where(lane < HEAD_SIZE // 2, peak, total)
    for k, (t, g) in enumerate(pairs):
        rows = slice(k * GROUP, (k + 1) * GROUP)
        values = jnp.dot(
            weights[rows].astype(jnp.bfloat16),
            cache_ref[1, t, :, columns[g]],
            preferred_element_type=jnp.float32,
        )
        for i in range(4):
            owner, row, pair = (t * 4 + i) * 4 + g // 2, (g % 2) * 2, slice(i * 2, i * 2 + 2)
            out_ref[owner, row : row + 2, :] = values[pair]
            out_ref[owner, row + 4 : row + 6, :] = stats[rows][pair]


PIECE = 5


def merge_kernel(parts_ref, out_ref):
    ny = parts_ref.shape[1]
    lane = lax.broadcasted_iota(jnp.int32, (1, HEAD_SIZE), 1)
    merged = []
    for y in range(ny):
        numerator, stats = parts_ref[:, y, :4, :], parts_ref[:, y, 4:, :]
        peak, total = stats[:, :, :1], stats[:, :, HEAD_SIZE // 2 : HEAD_SIZE // 2 + 1]
        top = jnp.max(peak, axis=0)
        factor = jnp.exp(peak - top[None])
        merged.append(
            (jnp.sum(numerator * factor, axis=0), top, jnp.sum(total * factor, axis=0))
        )
    copies = out_ref.shape[0] // (4 * PIECE)
    for w in range(4):
        stats = jnp.zeros((1, HEAD_SIZE), jnp.float32)
        for y, (_, top, total) in enumerate(merged):
            stats = jnp.where(lane >= 32 * y, top[w : w + 1], stats)
            stats = jnp.where(lane >= 32 * y + 16, total[w : w + 1], stats)
        piece = jnp.concatenate([part[w : w + 1] for part, _, _ in merged] + [stats], axis=0)
        for z in range(copies):
            row = (z * 4 + w) * PIECE
            out_ref[row : row + PIECE, :] = piece


def finish_kernel(parts_ref, out_ref):
    blocks = parts_ref.shape[0] // (4 * PIECE)
    rows = [None] * 16

    def across(row):
        return parts_ref[pl.ds(row, blocks, stride=4 * PIECE), :]

    for w in range(4):
        stats = across(w * PIECE + 4)
        for y in range(4):
            peak, total = stats[:, 32 * y : 32 * y + 1], stats[:, 32 * y + 16 : 32 * y + 17]
            factor = jnp.exp(peak - jnp.max(peak, axis=0, keepdims=True))
            total = jnp.sum(total * factor, axis=0, keepdims=True)
            values = jnp.sum(across(w * PIECE + y) * factor, axis=0, keepdims=True)
            rows[y * 4 + w] = values / total
    attention = jnp.concatenate(rows, axis=0).astype(jnp.bfloat16).astype(jnp.float32)
    for k in range(out_ref.shape[0]):
        out_ref[k] = attention


def out_kernel(heads_ref, weight_ref, out_ref):
    trajectories = out_ref.shape[1]
    for t in range(trajectories):
        total = jnp.zeros((heads_ref.shape[1], HEAD_SIZE), jnp.float32)
        for i in range(4):
            total += jnp.dot(
                heads_ref[t * 4 + i].astype(jnp.bfloat16),
                weight_ref[i * HEAD_SIZE : (i + 1) * HEAD_SIZE, :],
                preferred_element_type=jnp.float32,
            )
        out_ref[:, t, :] = total


def prefill_kernel(place_ref, *refs):
    tokens, refs = refs[:4], refs[4:]
    own_ref, other_ref, live_ref, starts_ref, cosine_ref, sine_ref, out_ref, total_ref = refs
    step = pl.program_id(0)

    @pl.when(step == 0)
    def _():
        total_ref[...] = jnp.zeros_like(total_ref)

    first = place_ref[2] == 0
    total = total_ref[...]
    for k, token_ref in enumerate(tokens):
        own, other = own_ref[k, 0], other_ref[k, 0]
        rows = jnp.concatenate(
            [jnp.where(first, own, other), jnp.where(first, other, own)], axis=0
        )
        total += jnp.dot(token_ref[...], rows, preferred_element_type=jnp.float32)
    total_ref[...] = total

    @pl.when(step == pl.num_programs(0) - 1)
    def _():
        prefixes = starts_ref.shape[0] // 2
        slot = lax.broadcasted_iota(jnp.int32, (SLOT, HEAD_SIZE), 0)
        front = lax.broadcasted_iota(jnp.int32, (SLOT, HEAD_SIZE), 1) < HEAD_SIZE // 2
        for i in range(prefixes):
            rows = slice(i * SLOT, (i + 1) * SLOT)
            plain = total_ref[rows, :]
            along, across = starts_ref[i : i + 1, :], starts_ref[prefixes + i : prefixes + i + 1, :]
            cosine = cosine_ref[...] * along - sine_ref[...] * across
            sine = sine_ref[...] * along + cosine_ref[...] * across
            swapped = pltpu.roll(plain, HEAD_SIZE // 2, 1)
            turned = plain * cosine + swapped * jnp.where(front, -sine, sine)
            kept = jnp.where(place_ref[3] > 0, turned, plain)
            out_ref[rows, :] = jnp.where(slot < live_ref[i], kept, 0.0).astype(jnp.bfloat16)


def prefill(place, tokens, own, other, live, starts, cosine, sine):
    rows, columns = tokens.shape[0], own.shape[-1]
    nx, nz = own.shape[:2]

    def token_block(k):
        def index(step, place):
            flipped = (step & 1) * 4 + (step & 2) + (step >> 2)
            return 0, (place[0] ^ flipped) * nx + ((place[1] + nx - k) & (nx - 1))

        return index

    def whole(array):
        return pl.BlockSpec(array.shape, lambda step, place: (0, 0))

    piece = pl.BlockSpec((nx, 1, *own.shape[2:]), lambda step, place: (0, step, 0, 0))
    result = jax.ShapeDtypeStruct((rows, columns), jnp.bfloat16)
    return pl.pallas_call(
        prefill_kernel,
        out_shape=result,
        grid_spec=pltpu.PrefetchScalarGridSpec(
            num_scalar_prefetch=1,
            grid=(nz,),
            in_specs=[pl.BlockSpec((rows, 2 * HEAD_SIZE), token_block(k)) for k in range(nx)]
            + [piece, piece, SMEM, whole(starts), whole(cosine), whole(sine)],
            out_specs=whole(result),
            scratch_shapes=[pltpu.VMEM((rows, columns), jnp.float32)],
        ),
        cost_estimate=pl.CostEstimate(
            flops=2 * 10**9, bytes_accessed=2 * tokens.size, transcendentals=0
        ),
    )(place, *([tokens] * nx), own, other, live, starts, cosine, sine)


VMEM = pl.BlockSpec(memory_space=pltpu.VMEM)
SMEM = pl.BlockSpec(memory_space=pltpu.SMEM)


def whole_call(kernel, shape, in_specs=(VMEM,), flops=10**7):
    return pl.pallas_call(
        kernel,
        out_shape=jax.ShapeDtypeStruct(shape, jnp.float32),
        in_specs=list(in_specs),
        out_specs=VMEM,
        cost_estimate=pl.CostEstimate(flops=flops, bytes_accessed=2**20, transcendentals=0),
    )


def shards(
    prefix_tokens,
    key_value_weight,
    prefix_lengths,
    start_offsets,
    queries,
    key_value_cache,
    cache_lengths,
    out_weight,
):
    columns = key_value_weight.shape[1]
    nz, nx, nc, ny, nw = (lax.axis_size(a) for a in ("z", "x", "c", "y", "w"))
    nxc, ngy = nx * nc, ny * nw

    blocks = key_value_weight[None]
    for far in (4, 2, 1):
        other = lax.ppermute(blocks, "z", [(i, i ^ far) for i in range(nz)])
        blocks = jnp.concatenate([blocks, other], axis=0)
    sides = [blocks]
    for k in range(1, nx):
        sides.append(lax.ppermute(blocks, "x", [(i, (i + k) % nx) for i in range(nx)]))
    own = jnp.stack(sides)
    other = lax.ppermute(own, "c", [(0, 1), (1, 0)])
    column = lax.axis_index(GY)
    place = jnp.stack(
        [*(lax.axis_index(a) for a in GX), KEY_VALUE_HEADS - column, lax.axis_index(GX)]
    )
    inverse, cosine, sine = turns()
    angles = start_offsets.astype(jnp.float32)[:, None] * inverse[None, :]
    starts = jnp.concatenate([jnp.cos(angles), jnp.sin(angles)], axis=0)
    prefix_kv = prefill(
        place, prefix_tokens, own, other, prefix_lengths, starts, cosine, sine
    )

    trajectories = queries.shape[0]
    parts = whole_call(
        block_kernel, (nxc * ny, 8, HEAD_SIZE), (SMEM, SMEM, VMEM, VMEM), flops=10**9
    )(place, cache_lengths, queries, key_value_cache)
    parts = swap(parts, ("x", "c", "y"))
    parts = whole_call(merge_kernel, (nz * nw * PIECE, HEAD_SIZE))(
        parts.reshape(nxc, ny, 8, HEAD_SIZE)
    )
    parts = swap(parts.reshape(nz * nw * PIECE, 1, HEAD_SIZE), ("z", "w"))
    attention = whole_call(finish_kernel, (nxc, ngy, HEAD_SIZE))(
        parts.reshape(nz * nw * PIECE, HEAD_SIZE)
    )
    heads = swap(attention, ("x", "c"))
    mixed = whole_call(out_kernel, (ngy, trajectories, columns), (VMEM, VMEM))(heads, out_weight)
    mixed = swap(mixed, GY)
    return (prefix_kv, jnp.sum(mixed, axis=0).astype(jnp.bfloat16))


def solution(mesh):
    finer = Mesh(mesh.devices.reshape(8, 4, 2, 4, 4), ("z", "x", "c", "y", "w"))
    return jax.shard_map(
        shards,
        mesh=finer,
        in_specs=(
            P(GX, None),
            P(GX, GY),
            P(GX),
            P(GX),
            P(GY, None),
            P(None, GY, GX, None),
            P(GY),
            P(GY, GX),
        ),
        out_specs=(P(GX, GY), P(GY, GX)),
        check_vma=False,
    )
```

```python
import jax
import jax.numpy as jnp
import numpy as np
from jax import lax
from jax.experimental import pallas as pl
from jax.experimental.pallas import tpu as pltpu
from jax.sharding import Mesh
from jax.sharding import PartitionSpec as P

QUERY_HEADS = 64
KEY_VALUE_HEADS = 8
HEAD_SIZE = 128
SLOT = 128
GX = ("z", "x", "c")
GY = ("y", "w")
GROUP = QUERY_HEADS // KEY_VALUE_HEADS

rope_base = 500000.0
masked_score = -1e30


def swap(pieces, axis):
    return lax.all_to_all(pieces, axis, 0, 0, tiled=True)


def turns():
    half_width = HEAD_SIZE // 2
    inverse = rope_base ** (-2.0 * (np.arange(HEAD_SIZE) % half_width) / HEAD_SIZE)
    angles = np.arange(SLOT)[:, None] * inverse[None, :]
    return tuple(np.float32(table) for table in (inverse, np.cos(angles), np.sin(angles)))


def block_kernel(place_ref, lengths_ref, query_ref, cache_ref, out_ref):
    trajectories, positions = cache_ref.shape[1], cache_ref.shape[2]
    start = place_ref[4] * positions
    pairs = [(t, g) for t in range(trajectories) for g in range(KEY_VALUE_HEADS)]
    columns = [slice(h * HEAD_SIZE, (h + 1) * HEAD_SIZE) for h in range(QUERY_HEADS)]
    queries = query_ref[...].astype(jnp.float32)
    order = [i + 4 * side for i in range(4) for side in range(2)]
    scores = jnp.concatenate(
        [
            lax.dot_general(
                jnp.concatenate(
                    [queries[t : t + 1, columns[g * GROUP + r]] for r in order], axis=0
                ).astype(jnp.bfloat16),
                cache_ref[0, t, :, columns[g]],
                (((1,), (1,)), ((), ())),
                preferred_element_type=jnp.float32,
            )
            for t, g in pairs
        ],
        axis=0,
    ) * HEAD_SIZE ** (-0.5)
    position = start + lax.broadcasted_iota(jnp.int32, (QUERY_HEADS, positions), 1)
    valid = jnp.concatenate([position < lengths_ref[t] for t in range(trajectories)], axis=0)
    peak = jnp.max(jnp.where(valid, scores, masked_score), axis=1, keepdims=True)
    weights = jnp.where(valid, jnp.exp(scores - peak), 0.0)
    total = jnp.sum(weights, axis=1, keepdims=True)
    lane = lax.broadcasted_iota(jnp.int32, weights.shape, 1)
    stats = jnp.where(lane < HEAD_SIZE // 2, peak, total)
    for k, (t, g) in enumerate(pairs):
        rows = slice(k * GROUP, (k + 1) * GROUP)
        values = jnp.dot(
            weights[rows].astype(jnp.bfloat16),
            cache_ref[1, t, :, columns[g]],
            preferred_element_type=jnp.float32,
        )
        for i in range(4):
            owner, row, pair = (t * 4 + i) * 4 + g // 2, (g % 2) * 2, slice(i * 2, i * 2 + 2)
            out_ref[owner, row : row + 2, :] = values[pair]
            out_ref[owner, row + 4 : row + 6, :] = stats[rows][pair]


PIECE = 5


def merge_kernel(parts_ref, out_ref):
    ny = parts_ref.shape[1]
    lane = lax.broadcasted_iota(jnp.int32, (1, HEAD_SIZE), 1)
    merged = []
    for y in range(ny):
        numerator, stats = parts_ref[:, y, :4, :], parts_ref[:, y, 4:, :]
        peak, total = stats[:, :, :1], stats[:, :, HEAD_SIZE // 2 : HEAD_SIZE // 2 + 1]
        top = jnp.max(peak, axis=0)
        factor = jnp.exp(peak - top[None])
        merged.append(
            (jnp.sum(numerator * factor, axis=0), top, jnp.sum(total * factor, axis=0))
        )
    copies = out_ref.shape[0] // (4 * PIECE)
    for w in range(4):
        stats = jnp.zeros((1, HEAD_SIZE), jnp.float32)
        for y, (_, top, total) in enumerate(merged):
            stats = jnp.where(lane >= 32 * y, top[w : w + 1], stats)
            stats = jnp.where(lane >= 32 * y + 16, total[w : w + 1], stats)
        piece = jnp.concatenate([part[w : w + 1] for part, _, _ in merged] + [stats], axis=0)
        for z in range(copies):
            row = (z * 4 + w) * PIECE
            out_ref[row : row + PIECE, :] = piece


def finish_kernel(parts_ref, out_ref):
    blocks = parts_ref.shape[0] // (4 * PIECE)
    rows = [None] * 16

    def across(row):
        return parts_ref[pl.ds(row, blocks, stride=4 * PIECE), :]

    for w in range(4):
        stats = across(w * PIECE + 4)
        for y in range(4):
            peak, total = stats[:, 32 * y : 32 * y + 1], stats[:, 32 * y + 16 : 32 * y + 17]
            factor = jnp.exp(peak - jnp.max(peak, axis=0, keepdims=True))
            total = jnp.sum(total * factor, axis=0, keepdims=True)
            values = jnp.sum(across(w * PIECE + y) * factor, axis=0, keepdims=True)
            rows[y * 4 + w] = values / total
    attention = jnp.concatenate(rows, axis=0).astype(jnp.bfloat16).astype(jnp.float32)
    for k in range(out_ref.shape[0]):
        out_ref[k] = attention


def out_kernel(heads_ref, weight_ref, out_ref):
    trajectories = out_ref.shape[1]
    for t in range(trajectories):
        total = jnp.zeros((heads_ref.shape[1], HEAD_SIZE), jnp.float32)
        for i in range(4):
            total += jnp.dot(
                heads_ref[t * 4 + i].astype(jnp.bfloat16),
                weight_ref[i * HEAD_SIZE : (i + 1) * HEAD_SIZE, :],
                preferred_element_type=jnp.float32,
            )
        out_ref[:, t, :] = total


def prefill_kernel(place_ref, *refs):
    tokens, refs = refs[:4], refs[4:]
    own_ref, other_ref, live_ref, starts_ref, cosine_ref, sine_ref, out_ref, total_ref = refs
    step = pl.program_id(0)

    @pl.when(step == 0)
    def _():
        total_ref[...] = jnp.zeros_like(total_ref)

    first = place_ref[2] == 0
    total = total_ref[...]
    for k, token_ref in enumerate(tokens):
        own, other = own_ref[k, 0], other_ref[k, 0]
        rows = jnp.concatenate(
            [jnp.where(first, own, other), jnp.where(first, other, own)], axis=0
        )
        total += jnp.dot(token_ref[...], rows, preferred_element_type=jnp.float32)
    total_ref[...] = total

    @pl.when(step == pl.num_programs(0) - 1)
    def _():
        prefixes = starts_ref.shape[0] // 2
        slot = lax.broadcasted_iota(jnp.int32, (SLOT, HEAD_SIZE), 0)
        front = lax.broadcasted_iota(jnp.int32, (SLOT, HEAD_SIZE), 1) < HEAD_SIZE // 2
        for i in range(prefixes):
            rows = slice(i * SLOT, (i + 1) * SLOT)
            plain = total_ref[rows, :]
            along, across = starts_ref[i : i + 1, :], starts_ref[prefixes + i : prefixes + i + 1, :]
            cosine = cosine_ref[...] * along - sine_ref[...] * across
            sine = sine_ref[...] * along + cosine_ref[...] * across
            swapped = pltpu.roll(plain, HEAD_SIZE // 2, 1)
            turned = plain * cosine + swapped * jnp.where(front, -sine, sine)
            kept = jnp.where(place_ref[3] > 0, turned, plain)
            out_ref[rows, :] = jnp.where(slot < live_ref[i], kept, 0.0).astype(jnp.bfloat16)


def prefill(place, tokens, own, other, live, starts, cosine, sine):
    rows, columns = tokens.shape[0], own.shape[-1]
    nx, nz = own.shape[:2]

    def token_block(k):
        def index(step, place):
            return 0, (place[0] ^ step) * nx + ((place[1] + nx - k) & (nx - 1))

        return index

    def whole(array):
        return pl.BlockSpec(array.shape, lambda step, place: (0, 0))

    piece = pl.BlockSpec((nx, 1, *own.shape[2:]), lambda step, place: (0, step, 0, 0))
    result = jax.ShapeDtypeStruct((rows, columns), jnp.bfloat16)
    return pl.pallas_call(
        prefill_kernel,
        out_shape=result,
        grid_spec=pltpu.PrefetchScalarGridSpec(
            num_scalar_prefetch=1,
            grid=(nz,),
            in_specs=[pl.BlockSpec((rows, 2 * HEAD_SIZE), token_block(k)) for k in range(nx)]
            + [piece, piece, SMEM, whole(starts), whole(cosine), whole(sine)],
            out_specs=whole(result),
            scratch_shapes=[pltpu.VMEM((rows, columns), jnp.float32)],
        ),
        cost_estimate=pl.CostEstimate(
            flops=2 * 10**9, bytes_accessed=2 * tokens.size, transcendentals=0
        ),
    )(place, *([tokens] * nx), own, other, live, starts, cosine, sine)


VMEM = pl.BlockSpec(memory_space=pltpu.VMEM)
SMEM = pl.BlockSpec(memory_space=pltpu.SMEM)


def whole_call(kernel, shape, in_specs=(VMEM,), flops=10**7):
    return pl.pallas_call(
        kernel,
        out_shape=jax.ShapeDtypeStruct(shape, jnp.float32),
        in_specs=list(in_specs),
        out_specs=VMEM,
        cost_estimate=pl.CostEstimate(flops=flops, bytes_accessed=2**20, transcendentals=0),
    )


def shards(
    prefix_tokens,
    key_value_weight,
    prefix_lengths,
    start_offsets,
    queries,
    key_value_cache,
    cache_lengths,
    out_weight,
):
    columns = key_value_weight.shape[1]
    nz, nx, nc, ny, nw = (lax.axis_size(a) for a in ("z", "x", "c", "y", "w"))
    nxc, ngy = nx * nc, ny * nw

    blocks = key_value_weight[None]
    other = lax.ppermute(blocks, "z", [(i, i ^ 1) for i in range(nz)])
    pairs = [jnp.concatenate([blocks, other], axis=0)]
    for far in (4, 6, 2):
        pairs.append(lax.ppermute(pairs[0], "z", [(i, i ^ far) for i in range(nz)]))
    blocks = jnp.stack([pairs[k] for k in (0, 3, 1, 2)]).reshape(nz, *key_value_weight.shape)
    sides = [blocks]
    for k in range(1, nx):
        sides.append(lax.ppermute(blocks, "x", [(i, (i + k) % nx) for i in range(nx)]))
    own = jnp.stack(sides)
    other = lax.ppermute(own, "c", [(0, 1), (1, 0)])
    column = lax.axis_index(GY)
    place = jnp.stack(
        [*(lax.axis_index(a) for a in GX), KEY_VALUE_HEADS - column, lax.axis_index(GX)]
    )
    inverse, cosine, sine = turns()
    angles = start_offsets.astype(jnp.float32)[:, None] * inverse[None, :]
    starts = jnp.concatenate([jnp.cos(angles), jnp.sin(angles)], axis=0)
    prefix_kv = prefill(
        place, prefix_tokens, own, other, prefix_lengths, starts, cosine, sine
    )

    trajectories = queries.shape[0]
    parts = whole_call(
        block_kernel, (nxc * ny, 8, HEAD_SIZE), (SMEM, SMEM, VMEM, VMEM), flops=10**9
    )(place, cache_lengths, queries, key_value_cache)
    parts = swap(parts, ("x", "c", "y"))
    parts = whole_call(merge_kernel, (nz * nw * PIECE, HEAD_SIZE))(
        parts.reshape(nxc, ny, 8, HEAD_SIZE)
    )
    parts = swap(parts.reshape(nz * nw * PIECE, 1, HEAD_SIZE), ("z", "w"))
    attention = whole_call(finish_kernel, (nxc, ngy, HEAD_SIZE))(
        parts.reshape(nz * nw * PIECE, HEAD_SIZE)
    )
    heads = swap(attention, ("x", "c"))
    mixed = whole_call(out_kernel, (ngy, trajectories, columns), (VMEM, VMEM))(heads, out_weight)
    mixed = swap(mixed, GY)
    return (prefix_kv, jnp.sum(mixed, axis=0).astype(jnp.bfloat16))


def solution(mesh):
    finer = Mesh(mesh.devices.reshape(8, 4, 2, 4, 4), ("z", "x", "c", "y", "w"))
    return jax.shard_map(
        shards,
        mesh=finer,
        in_specs=(
            P(GX, None),
            P(GX, GY),
            P(GX),
            P(GX),
            P(GY, None),
            P(None, GY, GX, None),
            P(GY),
            P(GY, GX),
        ),
        out_specs=(P(GX, GY), P(GY, GX)),
        check_vma=False,
    )
```

```python
import jax
import jax.numpy as jnp
import numpy as np
from jax import lax
from jax.experimental import pallas as pl
from jax.experimental.pallas import tpu as pltpu
from jax.sharding import Mesh
from jax.sharding import PartitionSpec as P

QUERY_HEADS = 64
KEY_VALUE_HEADS = 8
HEAD_SIZE = 128
SLOT = 128
GX = ("z", "x", "c")
GY = ("y", "w")
GROUP = QUERY_HEADS // KEY_VALUE_HEADS

rope_base = 500000.0
masked_score = -1e30


def swap(pieces, axis):
    return lax.all_to_all(pieces, axis, 0, 0, tiled=True)


def turns():
    half_width = HEAD_SIZE // 2
    inverse = rope_base ** (-2.0 * (np.arange(HEAD_SIZE) % half_width) / HEAD_SIZE)
    angles = np.arange(SLOT)[:, None] * inverse[None, :]
    return tuple(np.float32(table) for table in (inverse, np.cos(angles), np.sin(angles)))


def block_kernel(place_ref, lengths_ref, query_ref, cache_ref, out_ref):
    trajectories, positions = cache_ref.shape[1], cache_ref.shape[2]
    start = place_ref[4] * positions
    pairs = [(t, g) for t in range(trajectories) for g in range(KEY_VALUE_HEADS)]
    columns = [slice(h * HEAD_SIZE, (h + 1) * HEAD_SIZE) for h in range(QUERY_HEADS)]
    queries = query_ref[...].astype(jnp.float32)
    order = [i + 4 * side for i in range(4) for side in range(2)]
    scores = jnp.concatenate(
        [
            lax.dot_general(
                jnp.concatenate(
                    [queries[t : t + 1, columns[g * GROUP + r]] for r in order], axis=0
                ).astype(jnp.bfloat16),
                cache_ref[0, t, :, columns[g]],
                (((1,), (1,)), ((), ())),
                preferred_element_type=jnp.float32,
            )
            for t, g in pairs
        ],
        axis=0,
    ) * HEAD_SIZE ** (-0.5)
    position = start + lax.broadcasted_iota(jnp.int32, (QUERY_HEADS, positions), 1)
    valid = jnp.concatenate([position < lengths_ref[t] for t in range(trajectories)], axis=0)
    peak = jnp.max(jnp.where(valid, scores, masked_score), axis=1, keepdims=True)
    weights = jnp.where(valid, jnp.exp(scores - peak), 0.0)
    total = jnp.sum(weights, axis=1, keepdims=True)
    lane = lax.broadcasted_iota(jnp.int32, weights.shape, 1)
    stats = jnp.where(lane < HEAD_SIZE // 2, peak, total)
    for k, (t, g) in enumerate(pairs):
        rows = slice(k * GROUP, (k + 1) * GROUP)
        values = jnp.dot(
            weights[rows].astype(jnp.bfloat16),
            cache_ref[1, t, :, columns[g]],
            preferred_element_type=jnp.float32,
        )
        for i in range(4):
            owner, row, pair = (t * 4 + i) * 4 + g // 2, (g % 2) * 2, slice(i * 2, i * 2 + 2)
            out_ref[owner, row : row + 2, :] = values[pair]
            out_ref[owner, row + 4 : row + 6, :] = stats[rows][pair]


PIECE = 5


def merge_kernel(parts_ref, out_ref):
    ny = parts_ref.shape[1]
    lane = lax.broadcasted_iota(jnp.int32, (1, HEAD_SIZE), 1)
    merged = []
    for y in range(ny):
        numerator, stats = parts_ref[:, y, :4, :], parts_ref[:, y, 4:, :]
        peak, total = stats[:, :, :1], stats[:, :, HEAD_SIZE // 2 : HEAD_SIZE // 2 + 1]
        top = jnp.max(peak, axis=0)
        factor = jnp.exp(peak - top[None])
        merged.append(
            (jnp.sum(numerator * factor, axis=0), top, jnp.sum(total * factor, axis=0))
        )
    copies = out_ref.shape[0] // (4 * PIECE)
    for w in range(4):
        stats = jnp.zeros((1, HEAD_SIZE), jnp.float32)
        for y, (_, top, total) in enumerate(merged):
            stats = jnp.where(lane >= 32 * y, top[w : w + 1], stats)
            stats = jnp.where(lane >= 32 * y + 16, total[w : w + 1], stats)
        piece = jnp.concatenate([part[w : w + 1] for part, _, _ in merged] + [stats], axis=0)
        for z in range(copies):
            row = (z * 4 + w) * PIECE
            out_ref[row : row + PIECE, :] = piece


def finish_kernel(parts_ref, out_ref):
    blocks = parts_ref.shape[0] // (4 * PIECE)
    rows = [None] * 16

    def across(row):
        return parts_ref[pl.ds(row, blocks, stride=4 * PIECE), :]

    for w in range(4):
        stats = across(w * PIECE + 4)
        for y in range(4):
            peak, total = stats[:, 32 * y : 32 * y + 1], stats[:, 32 * y + 16 : 32 * y + 17]
            factor = jnp.exp(peak - jnp.max(peak, axis=0, keepdims=True))
            total = jnp.sum(total * factor, axis=0, keepdims=True)
            values = jnp.sum(across(w * PIECE + y) * factor, axis=0, keepdims=True)
            rows[y * 4 + w] = values / total
    attention = jnp.concatenate(rows, axis=0).astype(jnp.bfloat16).astype(jnp.float32)
    for k in range(out_ref.shape[0]):
        out_ref[k] = attention


def out_kernel(heads_ref, weight_ref, out_ref):
    trajectories = out_ref.shape[1]
    for t in range(trajectories):
        total = jnp.zeros((heads_ref.shape[1], HEAD_SIZE), jnp.float32)
        for i in range(4):
            total += jnp.dot(
                heads_ref[t * 4 + i].astype(jnp.bfloat16),
                weight_ref[i * HEAD_SIZE : (i + 1) * HEAD_SIZE, :],
                preferred_element_type=jnp.float32,
            )
        out_ref[:, t, :] = total


def prefill_kernel(place_ref, *refs):
    tokens, refs = refs[:4], refs[4:]
    own_ref, other_ref, live_ref, starts_ref, cosine_ref, sine_ref, out_ref, total_ref = refs
    step = pl.program_id(0)

    @pl.when(step == 0)
    def _():
        total_ref[...] = jnp.zeros_like(total_ref)

    first = place_ref[2] == 0
    total = total_ref[...]
    for k, token_ref in enumerate(tokens):
        own, other = own_ref[k, 0], other_ref[k, 0]
        rows = jnp.concatenate(
            [jnp.where(first, own, other), jnp.where(first, other, own)], axis=0
        )
        total += jnp.dot(token_ref[...], rows, preferred_element_type=jnp.float32)
    total_ref[...] = total

    @pl.when(step == pl.num_programs(0) - 1)
    def _():
        prefixes = starts_ref.shape[0] // 2
        slot = lax.broadcasted_iota(jnp.int32, (SLOT, HEAD_SIZE), 0)
        front = lax.broadcasted_iota(jnp.int32, (SLOT, HEAD_SIZE), 1) < HEAD_SIZE // 2
        for i in range(prefixes):
            rows = slice(i * SLOT, (i + 1) * SLOT)
            plain = total_ref[rows, :]
            along, across = starts_ref[i : i + 1, :], starts_ref[prefixes + i : prefixes + i + 1, :]
            cosine = cosine_ref[...] * along - sine_ref[...] * across
            sine = sine_ref[...] * along + cosine_ref[...] * across
            swapped = pltpu.roll(plain, HEAD_SIZE // 2, 1)
            turned = plain * cosine + swapped * jnp.where(front, -sine, sine)
            kept = jnp.where(place_ref[3] > 0, turned, plain)
            out_ref[rows, :] = jnp.where(slot < live_ref[i], kept, 0.0).astype(jnp.bfloat16)


def prefill(place, tokens, own, other, live, starts, cosine, sine):
    rows, columns = tokens.shape[0], own.shape[-1]
    nx, nz = own.shape[:2]

    def token_block(k):
        def index(step, place):
            return 0, (place[0] ^ ((step >> 1) + (step & 1) * 4)) * nx + ((place[1] + nx - k) & (nx - 1))

        return index

    def whole(array):
        return pl.BlockSpec(array.shape, lambda step, place: (0, 0))

    piece = pl.BlockSpec((nx, 1, *own.shape[2:]), lambda step, place: (0, step, 0, 0))
    result = jax.ShapeDtypeStruct((rows, columns), jnp.bfloat16)
    return pl.pallas_call(
        prefill_kernel,
        out_shape=result,
        grid_spec=pltpu.PrefetchScalarGridSpec(
            num_scalar_prefetch=1,
            grid=(nz,),
            in_specs=[pl.BlockSpec((rows, 2 * HEAD_SIZE), token_block(k)) for k in range(nx)]
            + [piece, piece, SMEM, whole(starts), whole(cosine), whole(sine)],
            out_specs=whole(result),
            scratch_shapes=[pltpu.VMEM((rows, columns), jnp.float32)],
        ),
        cost_estimate=pl.CostEstimate(
            flops=2 * 10**9, bytes_accessed=2 * tokens.size, transcendentals=0
        ),
    )(place, *([tokens] * nx), own, other, live, starts, cosine, sine)


VMEM = pl.BlockSpec(memory_space=pltpu.VMEM)
SMEM = pl.BlockSpec(memory_space=pltpu.SMEM)


def whole_call(kernel, shape, in_specs=(VMEM,), flops=10**7):
    return pl.pallas_call(
        kernel,
        out_shape=jax.ShapeDtypeStruct(shape, jnp.float32),
        in_specs=list(in_specs),
        out_specs=VMEM,
        cost_estimate=pl.CostEstimate(flops=flops, bytes_accessed=2**20, transcendentals=0),
    )


def shards(
    prefix_tokens,
    key_value_weight,
    prefix_lengths,
    start_offsets,
    queries,
    key_value_cache,
    cache_lengths,
    out_weight,
):
    columns = key_value_weight.shape[1]
    nz, nx, nc, ny, nw = (lax.axis_size(a) for a in ("z", "x", "c", "y", "w"))
    nxc, ngy = nx * nc, ny * nw

    blocks = key_value_weight[None]
    other = lax.ppermute(blocks, "z", [(i, i ^ 4) for i in range(nz)])
    pairs = [jnp.concatenate([blocks, other], axis=0)]
    for far in (1, 2, 3):
        pairs.append(lax.ppermute(pairs[0], "z", [(i, i ^ far) for i in range(nz)]))
    blocks = jnp.stack(pairs).reshape(nz, *key_value_weight.shape)
    sides = [blocks]
    for k in range(1, nx):
        sides.append(lax.ppermute(blocks, "x", [(i, (i + k) % nx) for i in range(nx)]))
    own = jnp.stack(sides)
    other = lax.ppermute(own, "c", [(0, 1), (1, 0)])
    column = lax.axis_index(GY)
    place = jnp.stack(
        [*(lax.axis_index(a) for a in GX), KEY_VALUE_HEADS - column, lax.axis_index(GX)]
    )
    inverse, cosine, sine = turns()
    angles = start_offsets.astype(jnp.float32)[:, None] * inverse[None, :]
    starts = jnp.concatenate([jnp.cos(angles), jnp.sin(angles)], axis=0)
    prefix_kv = prefill(
        place, prefix_tokens, own, other, prefix_lengths, starts, cosine, sine
    )

    trajectories = queries.shape[0]
    parts = whole_call(
        block_kernel, (nxc * ny, 8, HEAD_SIZE), (SMEM, SMEM, VMEM, VMEM), flops=10**9
    )(place, cache_lengths, queries, key_value_cache)
    parts = swap(parts, ("x", "c", "y"))
    parts = whole_call(merge_kernel, (nz * nw * PIECE, HEAD_SIZE))(
        parts.reshape(nxc, ny, 8, HEAD_SIZE)
    )
    parts = swap(parts.reshape(nz * nw * PIECE, 1, HEAD_SIZE), ("z", "w"))
    attention = whole_call(finish_kernel, (nxc, ngy, HEAD_SIZE))(
        parts.reshape(nz * nw * PIECE, HEAD_SIZE)
    )
    heads = swap(attention, ("x", "c"))
    mixed = whole_call(out_kernel, (ngy, trajectories, columns), (VMEM, VMEM))(heads, out_weight)
    mixed = swap(mixed, GY)
    return (prefix_kv, jnp.sum(mixed, axis=0).astype(jnp.bfloat16))


def solution(mesh):
    finer = Mesh(mesh.devices.reshape(8, 4, 2, 4, 4), ("z", "x", "c", "y", "w"))
    return jax.shard_map(
        shards,
        mesh=finer,
        in_specs=(
            P(GX, None),
            P(GX, GY),
            P(GX),
            P(GX),
            P(GY, None),
            P(None, GY, GX, None),
            P(GY),
            P(GY, GX),
        ),
        out_specs=(P(GX, GY), P(GY, GX)),
        check_vma=False,
    )
```

```python
import jax
import jax.numpy as jnp
import numpy as np
from jax import lax
from jax.experimental import pallas as pl
from jax.experimental.pallas import tpu as pltpu
from jax.sharding import Mesh
from jax.sharding import PartitionSpec as P

QUERY_HEADS = 64
KEY_VALUE_HEADS = 8
HEAD_SIZE = 128
SLOT = 128
GX = ("z", "x", "c")
GY = ("y", "w")
GROUP = QUERY_HEADS // KEY_VALUE_HEADS

rope_base = 500000.0
masked_score = -1e30


def swap(pieces, axis):
    return lax.all_to_all(pieces, axis, 0, 0, tiled=True)


def turns():
    half_width = HEAD_SIZE // 2
    inverse = rope_base ** (-2.0 * (np.arange(HEAD_SIZE) % half_width) / HEAD_SIZE)
    angles = np.arange(SLOT)[:, None] * inverse[None, :]
    return tuple(np.float32(table) for table in (inverse, np.cos(angles), np.sin(angles)))


def block_kernel(place_ref, lengths_ref, query_ref, cache_ref, out_ref):
    trajectories, positions = cache_ref.shape[1], cache_ref.shape[2]
    start = place_ref[4] * positions
    pairs = [(t, g) for t in range(trajectories) for g in range(KEY_VALUE_HEADS)]
    columns = [slice(h * HEAD_SIZE, (h + 1) * HEAD_SIZE) for h in range(QUERY_HEADS)]
    queries = query_ref[...].astype(jnp.float32)
    order = [i + 4 * side for i in range(4) for side in range(2)]
    scores = jnp.concatenate(
        [
            lax.dot_general(
                jnp.concatenate(
                    [queries[t : t + 1, columns[g * GROUP + r]] for r in order], axis=0
                ).astype(jnp.bfloat16),
                cache_ref[0, t, :, columns[g]],
                (((1,), (1,)), ((), ())),
                preferred_element_type=jnp.float32,
            )
            for t, g in pairs
        ],
        axis=0,
    ) * HEAD_SIZE ** (-0.5)
    position = start + lax.broadcasted_iota(jnp.int32, (QUERY_HEADS, positions), 1)
    valid = jnp.concatenate([position < lengths_ref[t] for t in range(trajectories)], axis=0)
    peak = jnp.max(jnp.where(valid, scores, masked_score), axis=1, keepdims=True)
    weights = jnp.where(valid, jnp.exp(scores - peak), 0.0)
    total = jnp.sum(weights, axis=1, keepdims=True)
    lane = lax.broadcasted_iota(jnp.int32, weights.shape, 1)
    stats = jnp.where(lane < HEAD_SIZE // 2, peak, total)
    for k, (t, g) in enumerate(pairs):
        rows = slice(k * GROUP, (k + 1) * GROUP)
        values = jnp.dot(
            weights[rows].astype(jnp.bfloat16),
            cache_ref[1, t, :, columns[g]],
            preferred_element_type=jnp.float32,
        )
        for i in range(4):
            owner, row, pair = (t * 4 + i) * 4 + g // 2, (g % 2) * 2, slice(i * 2, i * 2 + 2)
            out_ref[owner, row : row + 2, :] = values[pair]
            out_ref[owner, row + 4 : row + 6, :] = stats[rows][pair]


PIECE = 6


def merge_kernel(parts_ref, out_ref, rows_ref):
    ny = parts_ref.shape[1]
    lane = lax.broadcasted_iota(jnp.int32, (1, HEAD_SIZE), 1)
    merged = []
    for y in range(ny):
        numerator, stats = parts_ref[:, y, :4, :], parts_ref[:, y, 4:, :]
        peak, total = stats[:, :, :1], stats[:, :, HEAD_SIZE // 2 : HEAD_SIZE // 2 + 1]
        top = jnp.max(peak, axis=0)
        factor = jnp.exp(peak - top[None])
        total = jnp.sum(total * factor, axis=0)
        some = total > 0.0
        safe = jnp.where(some, total, 1.0)
        weight = jnp.where(some, top + jnp.log(safe), masked_score)
        high = weight.astype(jnp.bfloat16).astype(jnp.float32)
        middle = (weight - high).astype(jnp.bfloat16).astype(jnp.float32)
        low = weight - high - middle
        merged.append((jnp.sum(numerator * factor, axis=0) / safe, (high, middle, low)))
    copies = out_ref.shape[0] // (4 * PIECE)
    for w in range(4):
        stats = jnp.zeros((1, HEAD_SIZE), jnp.float32)
        for y, (_, split) in enumerate(merged):
            for k, part in enumerate(split):
                stats = jnp.where(lane >= 32 * y + 8 * k, part[w : w + 1], stats)
        rows = [part[w : w + 1] for part, _ in merged] + [stats, stats]
        piece = jnp.concatenate(rows, axis=0)
        for z in range(copies):
            row = (z * 4 + w) * PIECE
            rows_ref[row : row + PIECE, :] = piece
    out_ref[...] = rows_ref[...].astype(jnp.bfloat16)


def finish_kernel(parts_ref, out_ref, rows_ref):
    blocks = parts_ref.shape[0] // (4 * PIECE)
    rows = [None] * 16
    rows_ref[...] = parts_ref[...].astype(jnp.float32)

    def across(row):
        return rows_ref[pl.ds(row, blocks, stride=4 * PIECE), :]

    for w in range(4):
        stats = across(w * PIECE + 4)
        for y in range(4):
            high, middle, low = (stats[:, 32 * y + 8 * k : 32 * y + 8 * k + 1] for k in range(3))
            weight = high + middle + low
            factor = jnp.exp(weight - jnp.max(weight, axis=0, keepdims=True))
            total = jnp.sum(factor, axis=0, keepdims=True)
            values = jnp.sum(across(w * PIECE + y) * factor, axis=0, keepdims=True)
            rows[y * 4 + w] = values / total
    attention = jnp.concatenate(rows, axis=0).astype(jnp.bfloat16).astype(jnp.float32)
    for k in range(out_ref.shape[0]):
        out_ref[k] = attention


def out_kernel(heads_ref, weight_ref, out_ref):
    trajectories = out_ref.shape[1]
    for t in range(trajectories):
        total = jnp.zeros((heads_ref.shape[1], HEAD_SIZE), jnp.float32)
        for i in range(4):
            total += jnp.dot(
                heads_ref[t * 4 + i].astype(jnp.bfloat16),
                weight_ref[i * HEAD_SIZE : (i + 1) * HEAD_SIZE, :],
                preferred_element_type=jnp.float32,
            )
        out_ref[:, t, :] = total


def prefill_kernel(place_ref, *refs):
    tokens, refs = refs[:4], refs[4:]
    own_ref, other_ref, live_ref, starts_ref, cosine_ref, sine_ref, out_ref, total_ref = refs
    step = pl.program_id(0)

    @pl.when(step == 0)
    def _():
        total_ref[...] = jnp.zeros_like(total_ref)

    first = place_ref[2] == 0
    total = total_ref[...]
    for k, token_ref in enumerate(tokens):
        own, other = own_ref[k, 0], other_ref[k, 0]
        rows = jnp.concatenate(
            [jnp.where(first, own, other), jnp.where(first, other, own)], axis=0
        )
        total += jnp.dot(token_ref[...], rows, preferred_element_type=jnp.float32)
    total_ref[...] = total

    @pl.when(step == pl.num_programs(0) - 1)
    def _():
        prefixes = starts_ref.shape[0] // 2
        slot = lax.broadcasted_iota(jnp.int32, (SLOT, HEAD_SIZE), 0)
        front = lax.broadcasted_iota(jnp.int32, (SLOT, HEAD_SIZE), 1) < HEAD_SIZE // 2
        for i in range(prefixes):
            rows = slice(i * SLOT, (i + 1) * SLOT)
            plain = total_ref[rows, :]
            along, across = starts_ref[i : i + 1, :], starts_ref[prefixes + i : prefixes + i + 1, :]
            cosine = cosine_ref[...] * along - sine_ref[...] * across
            sine = sine_ref[...] * along + cosine_ref[...] * across
            swapped = pltpu.roll(plain, HEAD_SIZE // 2, 1)
            turned = plain * cosine + swapped * jnp.where(front, -sine, sine)
            kept = jnp.where(place_ref[3] > 0, turned, plain)
            out_ref[rows, :] = jnp.where(slot < live_ref[i], kept, 0.0).astype(jnp.bfloat16)


def prefill(place, tokens, own, other, live, starts, cosine, sine):
    rows, columns = tokens.shape[0], own.shape[-1]
    nx, nz = own.shape[:2]

    def token_block(k):
        def index(step, place):
            return 0, (place[0] ^ ((step >> 1) + (step & 1) * 4)) * nx + ((place[1] + nx - k) & (nx - 1))

        return index

    def whole(array):
        return pl.BlockSpec(array.shape, lambda step, place: (0, 0))

    piece = pl.BlockSpec((nx, 1, *own.shape[2:]), lambda step, place: (0, step, 0, 0))
    result = jax.ShapeDtypeStruct((rows, columns), jnp.bfloat16)
    return pl.pallas_call(
        prefill_kernel,
        out_shape=result,
        grid_spec=pltpu.PrefetchScalarGridSpec(
            num_scalar_prefetch=1,
            grid=(nz,),
            in_specs=[pl.BlockSpec((rows, 2 * HEAD_SIZE), token_block(k)) for k in range(nx)]
            + [piece, piece, SMEM, whole(starts), whole(cosine), whole(sine)],
            out_specs=whole(result),
            scratch_shapes=[pltpu.VMEM((rows, columns), jnp.float32)],
        ),
        cost_estimate=pl.CostEstimate(
            flops=2 * 10**9, bytes_accessed=2 * tokens.size, transcendentals=0
        ),
    )(place, *([tokens] * nx), own, other, live, starts, cosine, sine)


VMEM = pl.BlockSpec(memory_space=pltpu.VMEM)
SMEM = pl.BlockSpec(memory_space=pltpu.SMEM)


def whole_call(kernel, shape, in_specs=(VMEM,), flops=10**7, dtype=jnp.float32, scratch=()):
    return pl.pallas_call(
        kernel,
        out_shape=jax.ShapeDtypeStruct(shape, dtype),
        scratch_shapes=list(scratch),
        in_specs=list(in_specs),
        out_specs=VMEM,
        cost_estimate=pl.CostEstimate(flops=flops, bytes_accessed=2**20, transcendentals=0),
    )


def shards(
    prefix_tokens,
    key_value_weight,
    prefix_lengths,
    start_offsets,
    queries,
    key_value_cache,
    cache_lengths,
    out_weight,
):
    columns = key_value_weight.shape[1]
    nz, nx, nc, ny, nw = (lax.axis_size(a) for a in ("z", "x", "c", "y", "w"))
    nxc, ngy = nx * nc, ny * nw

    blocks = key_value_weight[None]
    other = lax.ppermute(blocks, "z", [(i, i ^ 4) for i in range(nz)])
    pairs = [jnp.concatenate([blocks, other], axis=0)]
    for far in (1, 2, 3):
        pairs.append(lax.ppermute(pairs[0], "z", [(i, i ^ far) for i in range(nz)]))
    blocks = jnp.stack(pairs).reshape(nz, *key_value_weight.shape)
    sides = [blocks]
    for k in range(1, nx):
        sides.append(lax.ppermute(blocks, "x", [(i, (i + k) % nx) for i in range(nx)]))
    own = jnp.stack(sides)
    other = lax.ppermute(own, "c", [(0, 1), (1, 0)])
    column = lax.axis_index(GY)
    place = jnp.stack(
        [*(lax.axis_index(a) for a in GX), KEY_VALUE_HEADS - column, lax.axis_index(GX)]
    )
    inverse, cosine, sine = turns()
    angles = start_offsets.astype(jnp.float32)[:, None] * inverse[None, :]
    starts = jnp.concatenate([jnp.cos(angles), jnp.sin(angles)], axis=0)
    prefix_kv = prefill(
        place, prefix_tokens, own, other, prefix_lengths, starts, cosine, sine
    )

    trajectories = queries.shape[0]
    parts = whole_call(
        block_kernel, (nxc * ny, 8, HEAD_SIZE), (SMEM, SMEM, VMEM, VMEM), flops=10**9
    )(place, cache_lengths, queries, key_value_cache)
    parts = swap(parts, ("x", "c", "y"))
    pieces = (nz * nw * PIECE, HEAD_SIZE)
    rows = (pltpu.VMEM(pieces, jnp.float32),)
    parts = whole_call(merge_kernel, pieces, dtype=jnp.bfloat16, scratch=rows)(
        parts.reshape(nxc, ny, 8, HEAD_SIZE)
    )
    parts = swap(parts.reshape(nz * nw * PIECE // 2, 2, HEAD_SIZE), ("z", "w"))
    attention = whole_call(finish_kernel, (nxc, ngy, HEAD_SIZE), scratch=rows)(
        parts.reshape(pieces)
    )
    heads = swap(attention, ("x", "c"))
    mixed = whole_call(out_kernel, (ngy, trajectories, columns), (VMEM, VMEM))(heads, out_weight)
    mixed = swap(mixed, GY)
    return (prefix_kv, jnp.sum(mixed, axis=0).astype(jnp.bfloat16))


def solution(mesh):
    finer = Mesh(mesh.devices.reshape(8, 4, 2, 4, 4), ("z", "x", "c", "y", "w"))
    return jax.shard_map(
        shards,
        mesh=finer,
        in_specs=(
            P(GX, None),
            P(GX, GY),
            P(GX),
            P(GX),
            P(GY, None),
            P(None, GY, GX, None),
            P(GY),
            P(GY, GX),
        ),
        out_specs=(P(GX, GY), P(GY, GX)),
        check_vma=False,
    )
```
